32 devices in a mesh: dp: 16 (over z, y, x), mp: 2 (over core).
Axes of the slice: x: 2, y: 2, z: 4, core: 2. Of those that a mesh axis runs over, the one named last changes fastest.
Arguments:
- hidden: bfloat16 [4096, 8192], P('dp', 'mp'), may hold values from -6 to 6
- w_key: bfloat16 [8192, 1024], P('mp', 'dp'), may hold values from -0.0625 to 0.0625
- w_value: bfloat16 [8192, 1024], P('mp', 'dp'), may hold values from -0.0625 to 0.0625
- queries: bfloat16 [4096, 8192], P('dp', 'mp'), may hold values from -150 to 150
- lengths: int32 [16], replicated, may hold values from 1 to 512, as said below
- seq_of_slot: int32 [32], replicated, may hold values from 0 to 15, as said below
- pos_of_slot: int32 [32], replicated, may hold values from 0 to 3, as said below
Outputs:
- context: bfloat16 [4096, 8192], P('dp', 'mp')
- key_cache: bfloat16 [16, 512, 1024], P('dp', None, 'mp')
- value_cache: bfloat16 [16, 512, 1024], P('dp', None, 'mp')
The draws below stay inside these ranges and needn't reach their ends.
Inputs may be any that keep to these rules, and one draw needn't show every extreme that they name: Sequence q has ceil(lengths[q] / 128) blocks, 1 to 4; some sequence has 4 full blocks. `seq_of_slot`: slots 2 i and 2 i + 1 belong to replica i. Every block of every sequence stands in exactly one slot. The blocks of one sequence stand on different replicas; the two slots of a replica hold blocks of different sequences; and for any two replicas A and B, at most one block on A is an earlier block of the same sequence as some block on B. `pos_of_slot`: given with seq_of_slot: the block index, from 0, of the block in each slot.
All inputs are finite; a program needn't handle non-finite values.
Results may differ from the reference program's by a relative error of at most 0.011.
Values may be sent and summed in bfloat16 or wider, within the bound.
A program may use at most 128 MiB of HBM per device.

```python
import math
import jax
import jax.numpy as jnp
from jax import lax

D = 8192
HQ = 64
KVH = 8
HD = 128
BLOCK = 128
MAXB = 4
SEQS = 16
TOKENS = 4096


def layout(key):
    total_seqs = SEQS
    groups = total_seqs // 4
    patterns = jnp.array([[4, 1, 1, 2], [3, 3, 1, 1], [2, 2, 2, 2], [4, 2, 1, 1], [3, 2, 2, 1], [1, 1, 3, 3], [2, 3, 1, 2]], jnp.int32)
    chosen = jax.random.randint(jax.random.fold_in(key, 101), (groups,), 0, 7)
    chosen = chosen.at[0].set(0)
    ranking = jax.random.randint(jax.random.fold_in(key, 102), (groups, 4), 0, 1 << 20) * 4 + jnp.arange(4, dtype=jnp.int32)[None, :]
    ordering = jnp.argsort(ranking, axis=1)
    counts = jnp.take_along_axis(patterns[chosen], ordering, axis=1).reshape(total_seqs)
    starts = jnp.cumsum(counts) - counts
    listed = jnp.arange(2 * total_seqs, dtype=jnp.int32)
    seq_listed = jnp.sum((starts[None, :] <= listed[:, None]).astype(jnp.int32), axis=1) - 1
    pos_listed = listed - starts[seq_listed]
    front_half = listed < total_seqs
    column = jnp.where(front_half, listed, (2 * total_seqs - listed) % total_seqs)
    shuffle = jax.random.permutation(jax.random.fold_in(key, 103), total_seqs)
    slot_index = shuffle[column] * 2 + jnp.where(front_half, 0, 1)
    seq_slots = jnp.zeros((2 * total_seqs,), jnp.int32).at[slot_index].set(seq_listed)
    pos_slots = jnp.zeros((2 * total_seqs,), jnp.int32).at[slot_index].set(pos_listed)
    tail_fill = jax.random.randint(jax.random.fold_in(key, 104), (total_seqs,), 1, BLOCK + 1)
    longest = jnp.argmax(counts == 4)
    tail_fill = tail_fill.at[longest].set(BLOCK)
    lengths = (counts - 1) * BLOCK + tail_fill
    return (lengths.astype(jnp.int32), seq_slots.astype(jnp.int32), pos_slots.astype(jnp.int32))


def draw_lengths(key, part):
    return layout(key)[0]


def draw_seq_of_slot(key, part):
    return layout(key)[1]


def draw_pos_of_slot(key, part):
    return layout(key)[2]


def draw_queries(key, part):
    shape = (TOKENS, HQ * HD)
    values = jnp.clip(jax.random.normal(jax.random.fold_in(key, 204), shape, jnp.float32), -6.0, 6.0)
    return values.astype(jnp.bfloat16)


def shard_levels(key, shape, shards, least, high):
    factor_of = 1.0
    for position, parts in shards:
        steps = jax.random.uniform(jax.random.fold_in(jax.random.fold_in(key, 6), position), (parts,), jnp.float32, least / len(shards), high / len(shards))
        factor_of = factor_of * jnp.repeat(jnp.exp(steps), shape[position] // parts).reshape((-1,) + (1,) * (len(shape) - 1 - position))
    return factor_of


def bell_draw(own_key, dims, deviation, most, cuts=(), kind=jnp.bfloat16):
    result = jax.random.normal(own_key, dims, jnp.float32) * deviation
    if len(cuts) > 0:
        result = shard_levels(own_key, dims, cuts, -0.22, 0.18) * result
    return jnp.clip(result, min=-most, max=most).astype(kind)


def setup_inputs(seed: int = 0) -> dict:
    seeds = jax.random.split(jax.random.key(seed), 8)
    return {
        "hidden": bell_draw(seeds[0], (TOKENS, D), 1.0, 6.0, ((0, 16), (1, 2))),
        "w_key": bell_draw(seeds[1], (D, KVH * HD), D ** -0.5, 0.0625, ((0, 2), (1, 16))),
        "w_value": bell_draw(seeds[2], (D, KVH * HD), D ** -0.5, 0.0625, ((0, 2), (1, 16))),
        "queries": draw_queries(jax.random.fold_in(seeds[7], 71), 0),
        "lengths": draw_lengths(jax.random.fold_in(seeds[7], 71), 0),
        "seq_of_slot": draw_seq_of_slot(jax.random.fold_in(seeds[7], 71), 0),
        "pos_of_slot": draw_pos_of_slot(jax.random.fold_in(seeds[7], 71), 0),
    }


def rotate(field, positions):
    halfway = field.shape[-1] // 2
    indices = jnp.arange(halfway, dtype=jnp.float32)
    frequency = jnp.exp(-(2.0 * indices / field.shape[-1]) * math.log(500000.0))
    angles = positions[:, None] * frequency[None, :]
    cosines = jnp.cos(angles)[:, None, :]
    sines = jnp.sin(angles)[:, None, :]
    front = field[..., :halfway]
    back = field[..., halfway:]
    return jnp.concatenate([front * cosines - back * sines, back * cosines + front * sines], axis=-1)

def reference(hidden, w_key, w_value, queries, lengths, seq_of_slot, pos_of_slot):
    total = hidden.shape[0]
    slot_count = seq_of_slot.shape[0]
    width = KVH * HD
    key_raw = jnp.dot(hidden, w_key, preferred_element_type=jnp.float32)
    value_rows = jnp.dot(hidden, w_value, preferred_element_type=jnp.float32).astype(jnp.bfloat16)
    rows = jnp.arange(total, dtype=jnp.int32)
    positions = pos_of_slot[rows // BLOCK] * BLOCK + rows % BLOCK
    key_rows = rotate(key_raw.reshape(total, KVH, HD), positions.astype(jnp.float32)).reshape(total, width).astype(jnp.bfloat16)
    slot_ids = jnp.arange(slot_count, dtype=jnp.int32)
    blocks = jnp.arange(MAXB, dtype=jnp.int32)
    sequences = jnp.arange(SEQS, dtype=jnp.int32)
    match = (seq_of_slot[None, None, :] == sequences[:, None, None]) & (pos_of_slot[None, None, :] == blocks[None, :, None])
    source = lax.optimization_barrier(jnp.sum(jnp.where(match, slot_ids[None, None, :], 0), axis=2)).astype(jnp.int32)
    span = MAXB * BLOCK
    cached = jnp.arange(span, dtype=jnp.int32)
    inside = cached[None, :] < lengths[:, None]

    def assemble(rows_all):
        blocked = rows_all.reshape(slot_count, BLOCK, width)[source].reshape(SEQS, span, width)
        return jnp.where(inside[:, :, None], blocked, jnp.zeros_like(blocked))
    key_cache = assemble(key_rows)
    value_cache = assemble(value_rows)
    ratio = HQ // KVH
    query_blocks = queries.reshape(slot_count, BLOCK, KVH, ratio, HD)
    offsets = jnp.arange(BLOCK, dtype=jnp.int32)

    def attend(slot_index):
        sequence = seq_of_slot[slot_index]
        length = lengths[sequence]
        query_pos = pos_of_slot[slot_index] * BLOCK + offsets
        allowed = (cached[None, :] <= query_pos[:, None]) & (cached[None, :] < length)
        key_here = key_cache[sequence].reshape(span, KVH, HD).astype(jnp.float32)
        value_here = value_cache[sequence].reshape(span, KVH, HD).astype(jnp.float32)
        scores = jnp.einsum('bgrd,cgd->grbc', query_blocks[slot_index].astype(jnp.float32), key_here) * (1.0 / math.sqrt(HD))
        scores = jnp.where(allowed[None, None], scores, -1e+30)
        largest = lax.optimization_barrier(jnp.max(scores, axis=-1, keepdims=True))
        weights = jnp.exp(scores - largest)
        probs = (weights / lax.optimization_barrier(jnp.sum(weights, axis=-1, keepdims=True))).astype(jnp.bfloat16)
        mixed = jnp.einsum('grbc,cgd->bgrd', probs.astype(jnp.float32), value_here)
        mixed = jnp.where((query_pos < length)[:, None, None, None], mixed, 0.0)
        return mixed.reshape(BLOCK, HQ * HD).astype(jnp.bfloat16)
    context = lax.map(attend, slot_ids).reshape(total, HQ * HD)
    return (context, key_cache, value_cache)
```

```python
import functools
import math

import jax
import jax.numpy as jnp
from jax import lax
from jax.experimental import pallas as pl
from jax.experimental.pallas import tpu as pltpu
from jax.sharding import PartitionSpec as P

HQ = 64
KVH = 8
HD = 128
BLOCK = 128
MAXB = 4


def rotate(field, positions):
    halfway = field.shape[-1] // 2
    indices = jnp.arange(halfway, dtype=jnp.float32)
    frequency = jnp.exp(-(2.0 * indices / field.shape[-1]) * math.log(500000.0))
    angles = positions[:, None] * frequency[None, :]
    cosines = jnp.cos(angles)[:, None, :]
    sines = jnp.sin(angles)[:, None, :]
    front = field[..., :halfway]
    back = field[..., halfway:]
    return jnp.concatenate(
        [front * cosines - back * sines, back * cosines + front * sines], axis=-1
    )


def shards(hidden, w_key, w_value, queries, lengths, seq_of_slot, pos_of_slot):
    replica = lax.axis_index("dp")
    token_rows = hidden.shape[0]
    local_slots = token_rows // BLOCK
    key_full, value_full = (
        lax.all_gather(w_key, "dp", axis=1, tiled=True),
        lax.all_gather(w_value, "dp", axis=1, tiled=True),
    )
    key_sum = jnp.dot(hidden, key_full, preferred_element_type=jnp.float32)
    value_sum = jnp.dot(hidden, value_full, preferred_element_type=jnp.float32)
    key_raw, value_raw = (
        lax.psum_scatter(key_sum, "mp", scatter_dimension=1, tiled=True),
        lax.psum_scatter(value_sum, "mp", scatter_dimension=1, tiled=True),
    )
    head_width = key_raw.shape[1]
    local_heads = head_width // HD
    my_seq = lax.dynamic_slice_in_dim(seq_of_slot, replica * local_slots, local_slots)
    my_pos = lax.dynamic_slice_in_dim(pos_of_slot, replica * local_slots, local_slots)
    offsets = jnp.arange(BLOCK, dtype=jnp.int32)
    query_pos = my_pos[:, None] * BLOCK + offsets[None, :]
    key_rows = rotate(
        key_raw.reshape(token_rows, local_heads, HD),
        query_pos.reshape(token_rows).astype(jnp.float32),
    )
    key_rows = key_rows.reshape(token_rows, head_width).astype(jnp.bfloat16)
    value_rows = value_raw.astype(jnp.bfloat16)
    payload = jnp.concatenate([key_rows, value_rows], axis=1).reshape(
        local_slots, BLOCK * 2 * head_width
    )
    blocks = jnp.arange(MAXB, dtype=jnp.int32)
    needed = (
        (seq_of_slot[None, None, :] == my_seq[:, None, None])
        & (pos_of_slot[None, None, :] == blocks[None, :, None])
        & (blocks[None, :, None] < my_pos[:, None, None])
    )
    owned = (seq_of_slot[None, :] == replica) & (pos_of_slot[None, :] == blocks[:, None])
    needed_pick = needed.astype(jnp.bfloat16)
    owned_pick = owned.astype(jnp.bfloat16)
    portion = lax.all_gather(payload, "dp", axis=0, tiled=True)
    earlier = jnp.einsum("smn,nx->smx", needed_pick, portion, preferred_element_type=jnp.float32)
    home_rows = jnp.dot(owned_pick, portion, preferred_element_type=jnp.float32)
    own_block = (blocks[None, :] == my_pos[:, None]).astype(jnp.float32)
    assembled = (earlier + own_block[:, :, None] * payload[:, None, :].astype(jnp.float32)).astype(
        jnp.bfloat16
    )
    span = MAXB * BLOCK
    assembled = assembled.reshape(local_slots, span, 2 * head_width)
    key_blocks = assembled[:, :, :head_width].reshape(local_slots, span, local_heads, HD)
    value_blocks = assembled[:, :, head_width:].reshape(local_slots, span, local_heads, HD)
    ratio = HQ // KVH
    query_blocks = queries.reshape(local_slots, BLOCK, local_heads, ratio, HD)
    scores = jnp.einsum(
        "sbgrd,scgd->sgrbc", query_blocks, key_blocks, preferred_element_type=jnp.float32
    ) * (1.0 / math.sqrt(HD))
    slot_lengths = lengths[my_seq]
    cached = jnp.arange(span, dtype=jnp.int32)
    allowed = (cached[None, None, :] <= query_pos[:, :, None]) & (
        cached[None, None, :] < slot_lengths[:, None, None]
    )
    scores = jnp.where(allowed[:, None, None], scores, -1e30)
    largest = jnp.max(scores, axis=-1, keepdims=True)
    weights = jnp.exp(scores - largest)
    probs = (weights / jnp.sum(weights, axis=-1, keepdims=True)).astype(jnp.bfloat16)
    mixed = jnp.einsum("sgrbc,scgd->sbgrd", probs, value_blocks, preferred_element_type=jnp.float32)
    valid = query_pos < slot_lengths[:, None]
    mixed = jnp.where(valid[:, :, None, None, None], mixed, 0.0)
    context = mixed.reshape(token_rows, local_heads * ratio * HD).astype(jnp.bfloat16)
    cache_rows = home_rows.reshape(span, 2 * head_width)
    own_length = lax.dynamic_slice_in_dim(lengths, replica, 1)[0]
    cache_rows = jnp.where((cached < own_length)[:, None], cache_rows, 0.0).astype(jnp.bfloat16)
    return (context, cache_rows[None, :, :head_width], cache_rows[None, :, head_width:])


MESH = pl.DeviceIdType.MESH
PAYLOAD_ORDERS = (("z", "x", "y"), ("y", "z", "x"), ("x", "y", "z"))
PAYLOAD_PARTS = (5, 3, 1)
HIDDEN_ORDERS = (("x", "y"), ("y", "x"))
HIDDEN_PARTS = (5, 3)
TILE = 16


def cut(rows, weights):
    tiles = rows // TILE
    sizes, done = [], 0
    for i, w in enumerate(weights):
        upto = tiles * sum(weights[: i + 1]) // sum(weights)
        sizes.append((done * TILE, (upto - done) * TILE))
        done = upto
    return sizes


def guarded(conditions, action):
    live = [c for c in conditions if c is not None]
    if not live:
        action()
        return
    test = live[0]
    for c in live[1:]:
        test = jnp.logical_and(test, c)
    pl.when(test)(action)


class Gather:
    def __init__(self, place, depth, view, orders, recv_sem, send_sem):
        self.place, self.depth, self.view = place, depth, view
        self.recv_sem, self.send_sem = recv_sem, send_sem
        self.sends = []
        found = []
        for part, order in enumerate(orders):
            reach = [(0, 0, 0, -1, 0)]
            for step, dim in enumerate(order):
                fresh = []
                for rx, ry, dz, _, hops in reach:
                    if dim == "x":
                        fresh.append((1, ry, dz, step, hops + 1))
                    elif dim == "y":
                        fresh.append((rx, 1, dz, step, hops + 1))
                    else:
                        for k in range(1, depth):
                            fresh.append((rx, ry, -k, step, hops + k))
                            fresh.append((rx, ry, k, step, hops + k))
                reach += fresh
            found += [(hops, part, order, step, rx, ry, dz) for rx, ry, dz, step, hops in reach]
        self.found = sorted(found, key=lambda f: f[0])
        self.slot = {(f[1], f[4], f[5], f[6]): i for i, f in enumerate(self.found)}

    @staticmethod
    def counts(depth, orders):
        pieces = sends = 0
        for order in orders:
            n = 1
            for dim in order:
                n *= 2 if dim in "xy" else 2 * depth - 1
            pieces += n
            sends += 3 * n
        return pieces, sends

    def exists(self, dz):
        z = self.place[2]
        if dz < 0:
            return z + dz >= 0
        if dz > 0:
            return z + dz < self.depth
        return None

    def ref(self, part, rx, ry, dz):
        x, y, z, _ = self.place
        ox = 1 - x if rx else x
        oy = 1 - y if ry else y
        return self.view(part, ox, oy, z + dz)

    def target(self, dim, sign):
        x, y, z, c = self.place
        if dim == "x":
            x = 1 - x
        elif dim == "y":
            y = 1 - y
        else:
            z = z + sign
        return ((z * 2 + y) * 2 + x, c)

    def send(self, part, rx, ry, dz, dim, sign):
        there = (part, rx ^ (dim == "x"), ry ^ (dim == "y"), dz - sign if dim == "z" else dz)
        if there not in self.slot:
            return
        z = self.place[2]
        conditions = [self.exists(dz)]
        if dim == "z":
            conditions.append(z + sign < self.depth if sign > 0 else z + sign >= 0)
        block = self.ref(part, rx, ry, dz)
        copy = pltpu.make_async_remote_copy(
            src_ref=block,
            dst_ref=block,
            send_sem=self.send_sem.at[len(self.sends)],
            recv_sem=self.recv_sem.at[self.slot[there]],
            device_id=self.target(dim, sign),
            device_id_type=MESH,
        )
        self.sends.append((conditions, copy))
        guarded(conditions, copy.start)

    def onward(self, entry):
        _, part, order, step, rx, ry, dz = entry
        if step >= 0 and order[step] == "z":
            self.send(part, rx, ry, dz, "z", 1 if dz < 0 else -1)
        for dim in order[step + 1 :]:
            if dim == "z":
                self.send(part, rx, ry, dz, "z", 1)
                self.send(part, rx, ry, dz, "z", -1)
            else:
                self.send(part, rx, ry, dz, dim, 0)

    def arrive(self, entry):
        _, part, order, step, rx, ry, dz = entry
        block = self.ref(part, rx, ry, dz)
        copy = pltpu.make_async_remote_copy(
            src_ref=block,
            dst_ref=block,
            send_sem=self.send_sem.at[0],
            recv_sem=self.recv_sem.at[self.slot[(part, rx, ry, dz)]],
            device_id=self.target("x", 0),
            device_id_type=MESH,
        )
        guarded([self.exists(dz)], copy.wait_recv)

    def own(self):
        return [f for f in self.found if f[0] == 0]

    def rest(self):
        return [f for f in self.found if f[0] > 0]

    def drain(self):
        for conditions, copy in self.sends:
            guarded(conditions, copy.wait_send)


def exchange_kernel(
    depth,
    hidden_ref,
    pack_ref,
    cos_ref,
    sin_ref,
    kv_ref,
    hid,
    packs,
    give,
    full,
    acc,
    peer,
    local_sem,
    swap_sem,
    peer_send,
    peer_recv,
    hid_recv,
    hid_send,
    w_recv,
    w_send,
    kv_recv,
    kv_send,
):
    me = lax.axis_index("dp")
    core = lax.axis_index("mp")
    x = me % 2
    y = (me // 2) % 2
    z = me // 4
    place = (x, y, z, core)
    rows = hidden_ref.shape[0]
    mine = y * 2 + x
    across = (z * 4 + y * 2 + (1 - x), core)
    along = (z * 4 + (1 - y) * 2 + x, core)
    other = (me, 1 - core)

    local = [
        pltpu.make_async_copy(hidden_ref, hid.at[mine], local_sem.at[0]),
        pltpu.make_async_copy(pack_ref.at[0], packs.at[z, x], local_sem.at[1]),
        pltpu.make_async_copy(pack_ref.at[1], give, local_sem.at[2]),
    ]
    for copy in local:
        copy.start()
    barrier = pltpu.get_barrier_semaphore()

    def greet(device):
        pl.semaphore_signal(barrier, inc=1, device_id=device, device_id_type=MESH)

    for device in (across, along, other):
        greet(device)
    pl.when(z > 0)(lambda: greet((me - 4, core)))
    pl.when(z < depth - 1)(lambda: greet((me + 4, core)))
    inner = jnp.logical_and(z > 0, z < depth - 1)
    pl.when(inner)(lambda: pl.semaphore_wait(barrier, 5))
    pl.when(jnp.logical_not(inner))(lambda: pl.semaphore_wait(barrier, 4 if depth > 1 else 3))
    for copy in local:
        copy.wait()

    swap = pltpu.make_async_remote_copy(
        src_ref=give,
        dst_ref=packs.at[z, x],
        send_sem=swap_sem.at[0],
        recv_sem=swap_sem.at[1],
        device_id=across,
        device_id_type=MESH,
    )
    swap.start()

    spans = cut(rows, HIDDEN_PARTS)

    def hid_view(part, ox, oy, oz):
        return hid.at[oy * 2 + ox, pl.ds(*spans[part])]

    def w_view(part, ox, oy, oz):
        half = x if part == 0 else 1 - x
        return packs.at[oz, half]

    hidden_gather = Gather(place, depth, hid_view, HIDDEN_ORDERS, hid_recv, hid_send)
    w_gather = Gather(place, depth, w_view, (("z",), ("z",)), w_recv, w_send)
    w_own = w_gather.own()
    w_gather.onward(w_own[0])
    for entry in hidden_gather.own():
        hidden_gather.onward(entry)
    swap.wait_recv()
    w_gather.onward(w_own[1])
    events = [(0.5 + f[0], 0, f) for f in w_gather.rest()]
    events += [(1.0 * f[0], 1, f) for f in hidden_gather.rest()]
    for _, which, entry in sorted(events, key=lambda e: e[0]):
        gather = (w_gather, hidden_gather)[which]
        gather.arrive(entry)
        gather.onward(entry)

    width = packs.shape[3] // 2
    span = packs.shape[2]
    for k in range(depth):
        h0 = packs[k, 0]
        h1 = packs[k, 1]
        columns = pl.ds(k * 2 * width, 2 * width)
        full[pl.ds(0, span), columns] = jnp.concatenate([h0[:, :width], h1[:, :width]], axis=1)
        full[pl.ds(span, span), columns] = jnp.concatenate([h0[:, width:], h1[:, width:]], axis=1)

    half_width = acc.shape[2]
    sends = []
    for i in range(4):
        block = pl.ds(i * rows, rows)
        for h in range(2):
            acc[h, block] = jnp.dot(
                hid[i],
                full[:, pl.ds(h * half_width, half_width)],
                preferred_element_type=jnp.float32,
            )
        copy = pltpu.make_async_remote_copy(
            src_ref=acc.at[1 - core, block],
            dst_ref=peer.at[block],
            send_sem=peer_send.at[i],
            recv_sem=peer_recv.at[i],
            device_id=other,
            device_id_type=MESH,
        )
        copy.start()
        sends.append(copy)

    heads = half_width // HD
    for i in range(4):
        sends[i].wait_recv()
        block = pl.ds(i * rows, rows)
        cosines = cos_ref[block]
        sines = sin_ref[block]
        for h in range(heads):
            columns = pl.ds(h * HD, HD)
            total = acc[core, block, columns] + peer[block, columns]
            turned = total * cosines + pltpu.roll(total, HD // 2, 1) * sines
            kv_ref[me, block, columns] = turned.astype(jnp.bfloat16)

    kv_spans = cut(kv_ref.shape[1], PAYLOAD_PARTS)

    def kv_view(part, ox, oy, oz):
        return kv_ref.at[(oz * 2 + oy) * 2 + ox, pl.ds(*kv_spans[part])]

    kv_gather = Gather(place, depth, kv_view, PAYLOAD_ORDERS, kv_recv, kv_send)
    for entry in kv_gather.own():
        kv_gather.onward(entry)
    for entry in kv_gather.rest():
        kv_gather.arrive(entry)
        kv_gather.onward(entry)

    swap.wait_send()
    for copy in sends:
        copy.wait_send()
    hidden_gather.drain()
    w_gather.drain()
    kv_gather.drain()


def attend_kernel(ratio, local_slots, tab_ref, q_ref, *refs):
    blocks, out_ref = refs[:MAXB], refs[MAXB]
    s = pl.program_id(0)
    length = tab_ref[local_slots * MAXB + s]
    start = tab_ref[local_slots * (MAXB + 1) + s] * BLOCK
    keys = jnp.concatenate([b[0, 0, 0] for b in blocks], axis=0)
    values = jnp.concatenate([b[0, 0, 1] for b in blocks], axis=0)
    span = keys.shape[0]
    row = start + lax.broadcasted_iota(jnp.int32, (BLOCK, span), 0)
    col = lax.broadcasted_iota(jnp.int32, (BLOCK, span), 1)
    allowed = (col <= row) & (col < length)
    valid = (start + lax.broadcasted_iota(jnp.int32, (BLOCK, HD), 0)) < length
    for r in range(ratio):
        columns = pl.ds(r * HD, HD)
        scores = lax.dot_general(
            q_ref[:, columns], keys, (((1,), (1,)), ((), ())), preferred_element_type=jnp.float32
        ) * (1.0 / math.sqrt(HD))
        scores = jnp.where(allowed, scores, -1e30)
        weights = jnp.exp(scores - jnp.max(scores, axis=1, keepdims=True))
        probs = (weights / jnp.sum(weights, axis=1, keepdims=True)).astype(jnp.bfloat16)
        mixed = jnp.dot(probs, values, preferred_element_type=jnp.float32)
        out_ref[:, columns] = jnp.where(valid, mixed, 0.0).astype(jnp.bfloat16)


def cache_kernel(local_heads, tab_ref, kv_ref, key_ref, value_ref):
    m = pl.program_id(0)
    length = tab_ref[MAXB]
    place = m * BLOCK + lax.broadcasted_iota(jnp.int32, (BLOCK, HD), 0)
    for g in range(local_heads):
        columns = pl.ds(g * HD, HD)
        inner = pl.ds(g // 2 * HD, HD)
        for which, out in ((0, key_ref), (1, value_ref)):
            block = kv_ref[0, g % 2, which, :, inner]
            out[0, :, columns] = jnp.where(place < length, block, jnp.zeros_like(block))


def fast_shards(hidden, w_key, w_value, queries, lengths, seq_of_slot, pos_of_slot):
    replica = lax.axis_index("dp")
    depth = lax.axis_size("dp") // 4
    rows, features = hidden.shape
    width = w_key.shape[1]
    plane = 4 * rows
    plane_slots = plane // BLOCK
    half_width = depth * width
    local_heads = 2 * half_width // HD
    x = replica % 2
    middle = features // 2
    k_pack = jnp.concatenate([w_key[:middle], w_key[middle:]], axis=1)
    v_pack = jnp.concatenate([w_value[:middle], w_value[middle:]], axis=1)
    pack = jnp.stack([jnp.where(x == 0, k_pack, v_pack), jnp.where(x == 0, v_pack, k_pack)])

    plane_pos = lax.dynamic_slice_in_dim(pos_of_slot, replica // 4 * plane_slots, plane_slots)
    positions = (plane_pos[:, None] * BLOCK + jnp.arange(BLOCK, dtype=jnp.int32)[None, :]).reshape(plane)
    lane = jnp.arange(HD, dtype=jnp.int32)
    indices = (lane % (HD // 2)).astype(jnp.float32)
    frequency = jnp.exp(-(2.0 * indices / HD) * math.log(500000.0))
    angles = positions.astype(jnp.float32)[:, None] * frequency[None, :]
    cosines = jnp.where(x == 0, jnp.cos(angles), 1.0)
    sines = jnp.sin(angles)
    sines = jnp.where(x == 0, jnp.where(lane[None, :] < HD // 2, -sines, sines), 0.0)

    hid_counts = Gather.counts(depth, HIDDEN_ORDERS)
    w_counts = Gather.counts(depth, (("z",), ("z",)))
    kv_counts = Gather.counts(depth, PAYLOAD_ORDERS)
    dma = pltpu.SemaphoreType.DMA
    vmem = pl.BlockSpec(memory_space=pltpu.VMEM)
    anywhere = pl.BlockSpec(memory_space=pl.ANY)
    kv = pl.pallas_call(
        functools.partial(exchange_kernel, depth),
        out_shape=jax.ShapeDtypeStruct((4 * depth, plane, half_width), jnp.bfloat16),
        in_specs=[anywhere, anywhere, vmem, vmem],
        out_specs=vmem,
        scratch_shapes=[
            pltpu.VMEM((4, rows, features), jnp.bfloat16),
            pltpu.VMEM((depth, 2, middle, 2 * width), jnp.bfloat16),
            pltpu.VMEM((middle, 2 * width), jnp.bfloat16),
            pltpu.VMEM((features, 2 * half_width), jnp.bfloat16),
            pltpu.VMEM((2, plane, half_width), jnp.float32),
            pltpu.VMEM((plane, half_width), jnp.float32),
            dma((3,)),
            dma((2,)),
            dma((4,)),
            dma((4,)),
            dma((hid_counts[0],)),
            dma((hid_counts[1],)),
            dma((w_counts[0],)),
            dma((w_counts[1],)),
            dma((kv_counts[0],)),
            dma((kv_counts[1],)),
        ],
        compiler_params=pltpu.CompilerParams(
            collective_id=0, has_side_effects=True, vmem_limit_bytes=60 * 2**20
        ),
    )(hidden, pack, cosines, sines)
    kv = kv.reshape(depth, 2, 2, plane, half_width)

    slots = rows // BLOCK
    my_seq = lax.dynamic_slice_in_dim(seq_of_slot, replica * slots, slots)
    my_pos = lax.dynamic_slice_in_dim(pos_of_slot, replica * slots, slots)
    wanted = jnp.concatenate([my_seq, replica[None].astype(jnp.int32)])
    blocks = jnp.arange(MAXB, dtype=jnp.int32)
    ids = jnp.arange(seq_of_slot.shape[0], dtype=jnp.int32)
    match = (seq_of_slot[None, None, :] == wanted[:, None, None]) & (
        pos_of_slot[None, None, :] == blocks[None, :, None]
    )
    source = jnp.sum(jnp.where(match, ids[None, None, :], 0), axis=2)
    bounds = jnp.sum(jnp.where(wanted[:, None] == jnp.arange(lengths.shape[0])[None, :], lengths[None, :], 0), axis=1)
    table = jnp.concatenate([source[:slots].reshape(-1), bounds[:slots], my_pos]).astype(jnp.int32)
    home = jnp.concatenate([source[slots], bounds[slots:]]).astype(jnp.int32)

    def block_spec(m):
        def index(s, g, tab):
            slot = tab[s * MAXB + m]
            return (slot // plane_slots, g % 2, 0, slot % plane_slots, g // 2)

        return pl.BlockSpec((1, 1, 2, BLOCK, HD), index)

    group = queries.shape[1] // local_heads
    context = pl.pallas_call(
        functools.partial(attend_kernel, group // HD, slots),
        out_shape=jax.ShapeDtypeStruct(queries.shape, jnp.bfloat16),
        grid_spec=pltpu.PrefetchScalarGridSpec(
            num_scalar_prefetch=1,
            grid=(slots, local_heads),
            in_specs=[pl.BlockSpec((BLOCK, group), lambda s, g, tab: (s, g))]
            + [block_spec(m) for m in range(MAXB)],
            out_specs=pl.BlockSpec((BLOCK, group), lambda s, g, tab: (s, g)),
        ),
    )(table, queries, *([kv] * MAXB))

    cache = jax.ShapeDtypeStruct((1, MAXB * BLOCK, local_heads * HD), jnp.bfloat16)
    cache_spec = pl.BlockSpec((1, BLOCK, local_heads * HD), lambda m, tab: (0, m, 0))
    key_cache, value_cache = pl.pallas_call(
        functools.partial(cache_kernel, local_heads),
        out_shape=(cache, cache),
        grid_spec=pltpu.PrefetchScalarGridSpec(
            num_scalar_prefetch=1,
            grid=(MAXB,),
            in_specs=[
                pl.BlockSpec(
                    (1, 2, 2, BLOCK, half_width),
                    lambda m, tab: (tab[m] // plane_slots, 0, 0, tab[m] % plane_slots, 0),
                )
            ],
            out_specs=(cache_spec, cache_spec),
        ),
    )(home, kv)
    return context, key_cache, value_cache


def suits(mesh):
    replicas, halves = mesh.shape["dp"], mesh.shape["mp"]
    return halves == 2 and replicas % 8 == 0 and KVH * HD == replicas * (HD // 2)


def solution(mesh):
    in_specs = (P("dp", "mp"), P("mp", "dp"), P("mp", "dp"), P("dp", "mp"), P(), P(), P())
    out_specs = (P("dp", "mp"), P("dp", None, "mp"), P("dp", None, "mp"))
    return jax.shard_map(fast_shards if suits(mesh) else shards, mesh=mesh, in_specs=in_specs, out_specs=out_specs, check_vma=False)
```

```python
import functools
import math

import jax
import jax.numpy as jnp
from jax import lax
from jax.experimental import pallas as pl
from jax.experimental.pallas import tpu as pltpu
from jax.sharding import PartitionSpec as P

HQ = 64
KVH = 8
HD = 128
BLOCK = 128
MAXB = 4


def rotate(field, positions):
    halfway = field.shape[-1] // 2
    indices = jnp.arange(halfway, dtype=jnp.float32)
    frequency = jnp.exp(-(2.0 * indices / field.shape[-1]) * math.log(500000.0))
    angles = positions[:, None] * frequency[None, :]
    cosines = jnp.cos(angles)[:, None, :]
    sines = jnp.sin(angles)[:, None, :]
    front = field[..., :halfway]
    back = field[..., halfway:]
    return jnp.concatenate(
        [front * cosines - back * sines, back * cosines + front * sines], axis=-1
    )


def shards(hidden, w_key, w_value, queries, lengths, seq_of_slot, pos_of_slot):
    replica = lax.axis_index("dp")
    token_rows = hidden.shape[0]
    local_slots = token_rows // BLOCK
    key_full, value_full = (
        lax.all_gather(w_key, "dp", axis=1, tiled=True),
        lax.all_gather(w_value, "dp", axis=1, tiled=True),
    )
    key_sum = jnp.dot(hidden, key_full, preferred_element_type=jnp.float32)
    value_sum = jnp.dot(hidden, value_full, preferred_element_type=jnp.float32)
    key_raw, value_raw = (
        lax.psum_scatter(key_sum, "mp", scatter_dimension=1, tiled=True),
        lax.psum_scatter(value_sum, "mp", scatter_dimension=1, tiled=True),
    )
    head_width = key_raw.shape[1]
    local_heads = head_width // HD
    my_seq = lax.dynamic_slice_in_dim(seq_of_slot, replica * local_slots, local_slots)
    my_pos = lax.dynamic_slice_in_dim(pos_of_slot, replica * local_slots, local_slots)
    offsets = jnp.arange(BLOCK, dtype=jnp.int32)
    query_pos = my_pos[:, None] * BLOCK + offsets[None, :]
    key_rows = rotate(
        key_raw.reshape(token_rows, local_heads, HD),
        query_pos.reshape(token_rows).astype(jnp.float32),
    )
    key_rows = key_rows.reshape(token_rows, head_width).astype(jnp.bfloat16)
    value_rows = value_raw.astype(jnp.bfloat16)
    payload = jnp.concatenate([key_rows, value_rows], axis=1).reshape(
        local_slots, BLOCK * 2 * head_width
    )
    blocks = jnp.arange(MAXB, dtype=jnp.int32)
    needed = (
        (seq_of_slot[None, None, :] == my_seq[:, None, None])
        & (pos_of_slot[None, None, :] == blocks[None, :, None])
        & (blocks[None, :, None] < my_pos[:, None, None])
    )
    owned = (seq_of_slot[None, :] == replica) & (pos_of_slot[None, :] == blocks[:, None])
    needed_pick = needed.astype(jnp.bfloat16)
    owned_pick = owned.astype(jnp.bfloat16)
    portion = lax.all_gather(payload, "dp", axis=0, tiled=True)
    earlier = jnp.einsum("smn,nx->smx", needed_pick, portion, preferred_element_type=jnp.float32)
    home_rows = jnp.dot(owned_pick, portion, preferred_element_type=jnp.float32)
    own_block = (blocks[None, :] == my_pos[:, None]).astype(jnp.float32)
    assembled = (earlier + own_block[:, :, None] * payload[:, None, :].astype(jnp.float32)).astype(
        jnp.bfloat16
    )
    span = MAXB * BLOCK
    assembled = assembled.reshape(local_slots, span, 2 * head_width)
    key_blocks = assembled[:, :, :head_width].reshape(local_slots, span, local_heads, HD)
    value_blocks = assembled[:, :, head_width:].reshape(local_slots, span, local_heads, HD)
    ratio = HQ // KVH
    query_blocks = queries.reshape(local_slots, BLOCK, local_heads, ratio, HD)
    scores = jnp.einsum(
        "sbgrd,scgd->sgrbc", query_blocks, key_blocks, preferred_element_type=jnp.float32
    ) * (1.0 / math.sqrt(HD))
    slot_lengths = lengths[my_seq]
    cached = jnp.arange(span, dtype=jnp.int32)
    allowed = (cached[None, None, :] <= query_pos[:, :, None]) & (
        cached[None, None, :] < slot_lengths[:, None, None]
    )
    scores = jnp.where(allowed[:, None, None], scores, -1e30)
    largest = jnp.max(scores, axis=-1, keepdims=True)
    weights = jnp.exp(scores - largest)
    probs = (weights / jnp.sum(weights, axis=-1, keepdims=True)).astype(jnp.bfloat16)
    mixed = jnp.einsum("sgrbc,scgd->sbgrd", probs, value_blocks, preferred_element_type=jnp.float32)
    valid = query_pos < slot_lengths[:, None]
    mixed = jnp.where(valid[:, :, None, None, None], mixed, 0.0)
    context = mixed.reshape(token_rows, local_heads * ratio * HD).astype(jnp.bfloat16)
    cache_rows = home_rows.reshape(span, 2 * head_width)
    own_length = lax.dynamic_slice_in_dim(lengths, replica, 1)[0]
    cache_rows = jnp.where((cached < own_length)[:, None], cache_rows, 0.0).astype(jnp.bfloat16)
    return (context, cache_rows[None, :, :head_width], cache_rows[None, :, head_width:])


MESH = pl.DeviceIdType.MESH
PAYLOAD_ORDERS = (("z", "x", "y"), ("y", "z", "x"), ("x", "y", "z"))
PAYLOAD_PARTS = (5, 3, 1)
HIDDEN_ORDERS = (("x", "y"), ("y", "x"))
HIDDEN_PARTS = (5, 3)
TILE = 16
PAIR = 2


def cut(rows, weights):
    tiles = rows // TILE
    sizes, done = [], 0
    for i, w in enumerate(weights):
        upto = tiles * sum(weights[: i + 1]) // sum(weights)
        sizes.append((done * TILE, (upto - done) * TILE))
        done = upto
    return sizes


def guarded(conditions, action):
    live = [c for c in conditions if c is not None]
    if not live:
        action()
        return
    test = live[0]
    for c in live[1:]:
        test = jnp.logical_and(test, c)
    pl.when(test)(action)


class Gather:
    def __init__(self, place, depth, view, orders, recv_sem, send_sem):
        self.place, self.depth, self.view = place, depth, view
        self.recv_sem, self.send_sem = recv_sem, send_sem
        self.sends = []
        found = []
        for part, order in enumerate(orders):
            reach = [(0, 0, 0, -1, 0)]
            for step, dim in enumerate(order):
                fresh = []
                for rx, ry, dz, _, hops in reach:
                    if dim == "x":
                        fresh.append((1, ry, dz, step, hops + 1))
                    elif dim == "y":
                        fresh.append((rx, 1, dz, step, hops + 1))
                    else:
                        for k in range(1, depth):
                            fresh.append((rx, ry, -k, step, hops + k))
                            fresh.append((rx, ry, k, step, hops + k))
                reach += fresh
            found += [(hops, part, order, step, rx, ry, dz) for rx, ry, dz, step, hops in reach]
        self.found = sorted(found, key=lambda f: (self.final(f), f[0], f[3] - len(f[2])))
        self.slot = {(f[1], f[4], f[5], f[6]): i for i, f in enumerate(self.found)}

    @staticmethod
    def final(entry):
        _, _, order, step, _, _, _ = entry
        return step == len(order) - 1 and order[step] != "z"

    @staticmethod
    def counts(depth, orders):
        pieces = sends = 0
        for order in orders:
            n = 1
            for dim in order:
                n *= 2 if dim in "xy" else 2 * depth - 1
            pieces += n
            sends += 3 * n
        return pieces, sends

    def exists(self, dz):
        z = self.place[2]
        if dz < 0:
            return z + dz >= 0
        if dz > 0:
            return z + dz < self.depth
        return None

    def ref(self, part, rx, ry, dz):
        x, y, z, _ = self.place
        ox = 1 - x if rx else x
        oy = 1 - y if ry else y
        return self.view(part, ox, oy, z + dz)

    def target(self, dim, sign):
        x, y, z, c = self.place
        if dim == "x":
            x = 1 - x
        elif dim == "y":
            y = 1 - y
        else:
            z = z + sign
        return ((z * 2 + y) * 2 + x, c)

    def send(self, part, rx, ry, dz, dim, sign):
        there = (part, rx ^ (dim == "x"), ry ^ (dim == "y"), dz - sign if dim == "z" else dz)
        if there not in self.slot:
            return
        z = self.place[2]
        conditions = [self.exists(dz)]
        if dim == "z":
            conditions.append(z + sign < self.depth if sign > 0 else z + sign >= 0)
        block = self.ref(part, rx, ry, dz)
        copy = pltpu.make_async_remote_copy(
            src_ref=block,
            dst_ref=block,
            send_sem=self.send_sem.at[len(self.sends)],
            recv_sem=self.recv_sem.at[self.slot[there]],
            device_id=self.target(dim, sign),
            device_id_type=MESH,
        )
        self.sends.append((conditions, copy))
        guarded(conditions, copy.start)

    def onward(self, entry):
        _, part, order, step, rx, ry, dz = entry
        if step >= 0 and order[step] == "z":
            self.send(part, rx, ry, dz, "z", 1 if dz < 0 else -1)
        for dim in order[step + 1 :]:
            if dim == "z":
                self.send(part, rx, ry, dz, "z", 1)
                self.send(part, rx, ry, dz, "z", -1)
            else:
                self.send(part, rx, ry, dz, dim, 0)

    def arrive(self, entry):
        _, part, order, step, rx, ry, dz = entry
        block = self.ref(part, rx, ry, dz)
        copy = pltpu.make_async_remote_copy(
            src_ref=block,
            dst_ref=block,
            send_sem=self.send_sem.at[0],
            recv_sem=self.recv_sem.at[self.slot[(part, rx, ry, dz)]],
            device_id=self.target("x", 0),
            device_id_type=MESH,
        )
        guarded([self.exists(dz)], copy.wait_recv)

    def own(self):
        return [f for f in self.found if f[0] == 0]

    def rest(self):
        return [f for f in self.found if f[0] > 0]

    def drain(self):
        for conditions, copy in self.sends:
            guarded(conditions, copy.wait_send)


def exchange_kernel(
    depth,
    hidden_ref,
    pack_ref,
    cos_ref,
    sin_ref,
    kv_ref,
    hid,
    packs,
    give,
    full,
    acc,
    peer,
    local_sem,
    swap_sem,
    peer_send,
    peer_recv,
    hid_recv,
    hid_send,
    w_recv,
    w_send,
    kv_recv,
    kv_send,
):
    me = lax.axis_index("dp")
    core = lax.axis_index("mp")
    x = me % 2
    y = (me // 2) % 2
    z = me // 4
    place = (x, y, z, core)
    rows = hidden_ref.shape[0]
    mine = y * 2 + x
    across = (z * 4 + y * 2 + (1 - x), core)
    along = (z * 4 + (1 - y) * 2 + x, core)
    other = (me, 1 - core)

    local = [
        pltpu.make_async_copy(hidden_ref, hid.at[mine], local_sem.at[0]),
        pltpu.make_async_copy(pack_ref.at[0], packs.at[z, x], local_sem.at[1]),
        pltpu.make_async_copy(pack_ref.at[1], give, local_sem.at[2]),
    ]
    for copy in local:
        copy.start()
    barrier = pltpu.get_barrier_semaphore()

    def greet(device):
        pl.semaphore_signal(barrier, inc=1, device_id=device, device_id_type=MESH)

    for device in (across, along, other):
        greet(device)
    pl.when(z > 0)(lambda: greet((me - 4, core)))
    pl.when(z < depth - 1)(lambda: greet((me + 4, core)))
    inner = jnp.logical_and(z > 0, z < depth - 1)
    pl.when(inner)(lambda: pl.semaphore_wait(barrier, 5))
    pl.when(jnp.logical_not(inner))(lambda: pl.semaphore_wait(barrier, 4 if depth > 1 else 3))
    for copy in local:
        copy.wait()

    swap = pltpu.make_async_remote_copy(
        src_ref=give,
        dst_ref=packs.at[z, x],
        send_sem=swap_sem.at[0],
        recv_sem=swap_sem.at[1],
        device_id=across,
        device_id_type=MESH,
    )
    swap.start()

    spans = cut(rows, HIDDEN_PARTS)

    def hid_view(part, ox, oy, oz):
        return hid.at[oy * 2 + ox, pl.ds(*spans[part])]

    def w_view(part, ox, oy, oz):
        half = x if part == 0 else 1 - x
        return packs.at[oz, half]

    hidden_gather = Gather(place, depth, hid_view, HIDDEN_ORDERS, hid_recv, hid_send)
    w_gather = Gather(place, depth, w_view, (("z",), ("z",)), w_recv, w_send)
    w_own = w_gather.own()
    w_gather.onward(w_own[0])
    for entry in hidden_gather.own():
        hidden_gather.onward(entry)
    swap.wait_recv()
    w_gather.onward(w_own[1])
    events = [(2.0 * f[0] - 1 + f[1], 0, f) for f in w_gather.rest()]
    events += [
        (100.0 if Gather.final(f) else 3.5 + 0.7 * f[1], 1, f) for f in hidden_gather.rest()
    ]
    for _, which, entry in sorted(events, key=lambda e: e[0]):
        gather = (w_gather, hidden_gather)[which]
        gather.arrive(entry)
        gather.onward(entry)

    width = packs.shape[3] // 2
    span = packs.shape[2]
    for k in range(depth):
        h0 = packs[k, 0]
        h1 = packs[k, 1]
        columns = pl.ds(k * 2 * width, 2 * width)
        full[pl.ds(0, span), columns] = jnp.concatenate([h0[:, :width], h1[:, :width]], axis=1)
        full[pl.ds(span, span), columns] = jnp.concatenate([h0[:, width:], h1[:, width:]], axis=1)

    half_width = acc.shape[2]
    sends = []
    for i in range(4):
        block = pl.ds(i * rows, rows)
        for h in range(2):
            acc[h, block] = jnp.dot(
                hid[i],
                full[:, pl.ds(h * half_width, half_width)],
                preferred_element_type=jnp.float32,
            )
        copy = pltpu.make_async_remote_copy(
            src_ref=acc.at[1 - core, block],
            dst_ref=peer.at[block],
            send_sem=peer_send.at[i],
            recv_sem=peer_recv.at[i],
            device_id=other,
            device_id_type=MESH,
        )
        copy.start()
        sends.append(copy)

    heads = half_width // HD
    for i in range(4):
        sends[i].wait_recv()
        block = pl.ds(i * rows, rows)
        cosines = cos_ref[block]
        sines = sin_ref[block]
        for h in range(heads):
            columns = pl.ds(h * HD, HD)
            total = acc[core, block, columns] + peer[block, columns]
            turned = total * cosines + pltpu.roll(total, HD // 2, 1) * sines
            kv_ref[me, block, columns] = turned.astype(jnp.bfloat16)

    kv_spans = cut(kv_ref.shape[1], PAYLOAD_PARTS)

    def kv_view(part, ox, oy, oz):
        return kv_ref.at[(oz * 2 + oy) * 2 + ox, pl.ds(*kv_spans[part])]

    kv_gather = Gather(place, depth, kv_view, PAYLOAD_ORDERS, kv_recv, kv_send)
    for entry in kv_gather.own():
        kv_gather.onward(entry)
    for entry in kv_gather.rest():
        kv_gather.arrive(entry)
        kv_gather.onward(entry)

    swap.wait_send()
    for copy in sends:
        copy.wait_send()
    hidden_gather.drain()
    w_gather.drain()
    kv_gather.drain()


def attend_kernel(ratio, local_slots, tab_ref, q_ref, *refs):
    blocks, out_ref = refs[:MAXB], refs[MAXB]
    s = pl.program_id(0)
    length = tab_ref[local_slots * MAXB + s]
    start = tab_ref[local_slots * (MAXB + 1) + s] * BLOCK
    keys = jnp.concatenate([b[0, 0, 0] for b in blocks], axis=0)
    values = jnp.concatenate([b[0, 0, 1] for b in blocks], axis=0)
    span = keys.shape[0]
    row = start + lax.broadcasted_iota(jnp.int32, (BLOCK, span), 0)
    col = lax.broadcasted_iota(jnp.int32, (BLOCK, span), 1)
    bias = jnp.where((col <= row) & (col < length), 0.0, -1e30)
    bias = jnp.concatenate([bias] * PAIR, axis=0)
    valid = (start + lax.broadcasted_iota(jnp.int32, (BLOCK, HD), 0)) < length
    for r in range(0, ratio, PAIR):
        q = jnp.concatenate([q_ref[:, pl.ds((r + i) * HD, HD)] for i in range(PAIR)], axis=0)
        scores = lax.dot_general(
            q, keys, (((1,), (1,)), ((), ())), preferred_element_type=jnp.float32
        )
        scores = scores + bias
        largest = jnp.max(scores, axis=1, keepdims=True)
        weights = jnp.exp2((scores - largest) * (math.log2(math.e) / math.sqrt(HD)))
        scale = 1.0 / jnp.sum(weights, axis=1, keepdims=True)
        mixed = jnp.dot(weights.astype(jnp.bfloat16), values, preferred_element_type=jnp.float32)
        mixed = mixed * scale
        for i in range(PAIR):
            part = jnp.where(valid, mixed[i * BLOCK : (i + 1) * BLOCK], 0.0)
            out_ref[:, pl.ds((r + i) * HD, HD)] = part.astype(jnp.bfloat16)


def cache_kernel(local_heads, tab_ref, kv_ref, key_ref, value_ref):
    m = pl.program_id(0)
    length = tab_ref[MAXB]
    place = m * BLOCK + lax.broadcasted_iota(jnp.int32, (BLOCK, HD), 0)
    for g in range(local_heads):
        columns = pl.ds(g * HD, HD)
        inner = pl.ds(g // 2 * HD, HD)
        for which, out in ((0, key_ref), (1, value_ref)):
            block = kv_ref[0, g % 2, which, :, inner]
            out[0, :, columns] = jnp.where(place < length, block, jnp.zeros_like(block))


def fast_shards(hidden, w_key, w_value, queries, lengths, seq_of_slot, pos_of_slot):
    replica = lax.axis_index("dp")
    depth = lax.axis_size("dp") // 4
    rows, features = hidden.shape
    width = w_key.shape[1]
    plane = 4 * rows
    plane_slots = plane // BLOCK
    half_width = depth * width
    local_heads = 2 * half_width // HD
    x = replica % 2
    middle = features // 2
    k_pack = jnp.concatenate([w_key[:middle], w_key[middle:]], axis=1)
    v_pack = jnp.concatenate([w_value[:middle], w_value[middle:]], axis=1)
    pack = jnp.stack([jnp.where(x == 0, k_pack, v_pack), jnp.where(x == 0, v_pack, k_pack)])

    plane_pos = lax.dynamic_slice_in_dim(pos_of_slot, replica // 4 * plane_slots, plane_slots)
    positions = (plane_pos[:, None] * BLOCK + jnp.arange(BLOCK, dtype=jnp.int32)[None, :]).reshape(plane)
    lane = jnp.arange(HD, dtype=jnp.int32)
    indices = (lane % (HD // 2)).astype(jnp.float32)
    frequency = jnp.exp(-(2.0 * indices / HD) * math.log(500000.0))
    angles = positions.astype(jnp.float32)[:, None] * frequency[None, :]
    cosines = jnp.where(x == 0, jnp.cos(angles), 1.0)
    sines = jnp.sin(angles)
    sines = jnp.where(x == 0, jnp.where(lane[None, :] < HD // 2, -sines, sines), 0.0)

    hid_counts = Gather.counts(depth, HIDDEN_ORDERS)
    w_counts = Gather.counts(depth, (("z",), ("z",)))
    kv_counts = Gather.counts(depth, PAYLOAD_ORDERS)
    dma = pltpu.SemaphoreType.DMA
    vmem = pl.BlockSpec(memory_space=pltpu.VMEM)
    anywhere = pl.BlockSpec(memory_space=pl.ANY)
    kv = pl.pallas_call(
        functools.partial(exchange_kernel, depth),
        out_shape=jax.ShapeDtypeStruct((4 * depth, plane, half_width), jnp.bfloat16),
        in_specs=[anywhere, anywhere, vmem, vmem],
        out_specs=vmem,
        scratch_shapes=[
            pltpu.VMEM((4, rows, features), jnp.bfloat16),
            pltpu.VMEM((depth, 2, middle, 2 * width), jnp.bfloat16),
            pltpu.VMEM((middle, 2 * width), jnp.bfloat16),
            pltpu.VMEM((features, 2 * half_width), jnp.bfloat16),
            pltpu.VMEM((2, plane, half_width), jnp.float32),
            pltpu.VMEM((plane, half_width), jnp.float32),
            dma((3,)),
            dma((2,)),
            dma((4,)),
            dma((4,)),
            dma((hid_counts[0],)),
            dma((hid_counts[1],)),
            dma((w_counts[0],)),
            dma((w_counts[1],)),
            dma((kv_counts[0],)),
            dma((kv_counts[1],)),
        ],
        compiler_params=pltpu.CompilerParams(
            collective_id=0, has_side_effects=True, vmem_limit_bytes=60 * 2**20
        ),
    )(hidden, pack, cosines, sines)
    kv = kv.reshape(depth, 2, 2, plane, half_width)

    slots = rows // BLOCK
    my_seq = lax.dynamic_slice_in_dim(seq_of_slot, replica * slots, slots)
    my_pos = lax.dynamic_slice_in_dim(pos_of_slot, replica * slots, slots)
    wanted = jnp.concatenate([my_seq, replica[None].astype(jnp.int32)])
    blocks = jnp.arange(MAXB, dtype=jnp.int32)
    ids = jnp.arange(seq_of_slot.shape[0], dtype=jnp.int32)
    match = (seq_of_slot[None, None, :] == wanted[:, None, None]) & (
        pos_of_slot[None, None, :] == blocks[None, :, None]
    )
    source = jnp.sum(jnp.where(match, ids[None, None, :], 0), axis=2)
    bounds = jnp.sum(jnp.where(wanted[:, None] == jnp.arange(lengths.shape[0])[None, :], lengths[None, :], 0), axis=1)
    table = jnp.concatenate([source[:slots].reshape(-1), bounds[:slots], my_pos]).astype(jnp.int32)
    home = jnp.concatenate([source[slots], bounds[slots:]]).astype(jnp.int32)

    def block_spec(m):
        def index(s, g, tab):
            slot = tab[s * MAXB + m]
            return (slot // plane_slots, g % 2, 0, slot % plane_slots, g // 2)

        return pl.BlockSpec((1, 1, 2, BLOCK, HD), index)

    group = queries.shape[1] // local_heads
    context = pl.pallas_call(
        functools.partial(attend_kernel, group // HD, slots),
        out_shape=jax.ShapeDtypeStruct(queries.shape, jnp.bfloat16),
        grid_spec=pltpu.PrefetchScalarGridSpec(
            num_scalar_prefetch=1,
            grid=(slots, local_heads),
            in_specs=[pl.BlockSpec((BLOCK, group), lambda s, g, tab: (s, g))]
            + [block_spec(m) for m in range(MAXB)],
            out_specs=pl.BlockSpec((BLOCK, group), lambda s, g, tab: (s, g)),
        ),
    )(table, queries, *([kv] * MAXB))

    cache = jax.ShapeDtypeStruct((1, MAXB * BLOCK, local_heads * HD), jnp.bfloat16)
    cache_spec = pl.BlockSpec((1, BLOCK, local_heads * HD), lambda m, tab: (0, m, 0))
    key_cache, value_cache = pl.pallas_call(
        functools.partial(cache_kernel, local_heads),
        out_shape=(cache, cache),
        grid_spec=pltpu.PrefetchScalarGridSpec(
            num_scalar_prefetch=1,
            grid=(MAXB,),
            in_specs=[
                pl.BlockSpec(
                    (1, 2, 2, BLOCK, half_width),
                    lambda m, tab: (tab[m] // plane_slots, 0, 0, tab[m] % plane_slots, 0),
                )
            ],
            out_specs=(cache_spec, cache_spec),
        ),
    )(home, kv)
    return context, key_cache, value_cache


def suits(mesh):
    replicas, halves = mesh.shape["dp"], mesh.shape["mp"]
    return halves == 2 and replicas % 8 == 0 and KVH * HD == replicas * (HD // 2)


def solution(mesh):
    in_specs = (P("dp", "mp"), P("mp", "dp"), P("mp", "dp"), P("dp", "mp"), P(), P(), P())
    out_specs = (P("dp", "mp"), P("dp", None, "mp"), P("dp", None, "mp"))
    return jax.shard_map(fast_shards if suits(mesh) else shards, mesh=mesh, in_specs=in_specs, out_specs=out_specs, check_vma=False)
```
